512 devices in a mesh: blk: 64 (over z, x_lo, core), strip: 8 (over x_hi, y).
Axes of the slice: x: 4 (x_hi: 2, x_lo: 2; x = x_hi * 2 + x_lo), y: 4, z: 16, core: 2. Of those that a mesh axis runs over, the one named last changes fastest.
Arguments:
- points: bfloat16 [81920, 64], P(('blk', 'strip')), may hold values from -6 to 6
- task_ids: int32 [81920], P(('blk', 'strip')), may hold values from 0 to 3
- rhs: bfloat16 [81920, 32], P(('blk', 'strip')), may hold values from -6 to 6
- length_scales: float32 [64], replicated, may hold values from 2 to 5
- coregion: float32 [4, 4], replicated, may hold values from -4 to 6, as said below
- noise: float32 [1], replicated, may hold values from 0.2 to 1
Outputs:
- product: float32 [81920, 32], P(('blk', 'strip'))
The draws below stay inside these ranges and needn't reach their ends.
Inputs may be any that keep to these rules, and one draw needn't show every extreme that they name: coregion is symmetric positive definite.
All inputs are finite; a program needn't handle non-finite values.
Results may differ from the reference program's by a relative error of at most 0.0041.
Values may be sent and summed in bfloat16 or wider, within the bound.
No kernel may reach another device: no remote copies, remote signals or barrier semaphores. Data moves between devices by JAX's collectives and lax.ppermute only.
A program may use at most 64 MiB of HBM per device.

```python
import math
import jax
import jax.numpy as jnp
from jax import lax

FEAT = 64
RHS = 32
TASKS = 4
BLK_PTS = 1280
POINTS = 81920
N_BLK = 64


def draw_coregion(key, part):
    first, second = jax.random.split(jax.random.fold_in(key, 11))
    loading = jnp.clip(jax.random.normal(first, (TASKS, TASKS), jnp.float32), -2.0, 2.0) * 0.5
    extra = jax.random.uniform(second, (TASKS,), jnp.float32, 0.5, 1.5)
    return jnp.dot(loading, loading.T, precision=lax.Precision.HIGHEST) + jnp.diag(extra)


def touch_ends(array, key, least, high):
    place = [jax.random.randint(jax.random.fold_in(key, axis), (), 0, length) for axis, length in enumerate(array.shape)]
    widest = array.shape.index(max(array.shape))
    next_to = place[:widest] + [(place[widest] + 1) % array.shape[widest]] + place[widest + 1:]
    return array.at[tuple(place)].set(least).at[tuple(next_to)].set(high)


def block_scale(rng, shape, cuts, least, top_value):
    gain = 1.0
    for position, shards_of in cuts:
        steps = jax.random.uniform(jax.random.fold_in(jax.random.fold_in(rng, 6), position), (shards_of,), jnp.float32, least / len(cuts), top_value / len(cuts))
        gain = gain * jnp.repeat(jnp.exp(steps), shape[position] // shards_of).reshape((-1,) + (1,) * (len(shape) - 1 - position))
    return gain


def gaussian(own_key, extent, deviation, bound, cuts=(), held_as=jnp.bfloat16):
    level = block_scale(own_key, extent, cuts, -0.22, 0.18) if cuts else 1.0
    values = jax.random.normal(own_key, extent, jnp.float32) * deviation * level
    return jnp.minimum(jnp.maximum(values, -bound), bound).astype(held_as)


def setup_inputs(seed: int = 0) -> dict:
    keys = jax.random.split(jax.random.key(seed), 7)
    points = gaussian(keys[0], (POINTS, FEAT), 1.0, 6.0, ((0, 512),))
    task_ids = touch_ends(jax.random.randint(keys[1], (POINTS,), 0, TASKS), jax.random.fold_in(keys[1], 1), 0, TASKS - 1).astype(jnp.int32)
    rhs = gaussian(keys[2], (POINTS, RHS), 1.0, 6.0, ((0, 512),))
    length_scales = jnp.clip(jnp.exp(jax.random.uniform(keys[3], (FEAT,), jnp.float32, math.log(2.0), math.log(5.0))), 2.0, 5.0)
    coregion = draw_coregion(jax.random.fold_in(keys[6], 71), 0)
    noise = jnp.clip(jax.random.uniform(keys[5], (1,), jnp.float32, 0.2, 1.0), 0.2, 1.0)
    return dict(points=points, task_ids=task_ids, rhs=rhs, length_scales=length_scales, coregion=coregion, noise=noise)


def reference(points, task_ids, rhs, length_scales, coregion, noise):
    scaled = (points.astype(jnp.float32) / length_scales[None, :]).astype(jnp.bfloat16)
    widened = lax.optimization_barrier(scaled).astype(jnp.float32)
    norms = lax.optimization_barrier(jnp.sum(widened * widened, axis=1))
    rhs_wide = rhs.astype(jnp.float32)
    row_factors = coregion[task_ids]
    row_step = BLK_PTS // 4

    def one_block(start):
        rows = lax.dynamic_slice_in_dim(widened, start, row_step, 0)
        row_norms = lax.dynamic_slice_in_dim(norms, start, row_step, 0)
        factors = lax.dynamic_slice_in_dim(row_factors, start, row_step, 0)
        crossed = jnp.dot(rows, widened.T, precision=lax.Precision.HIGHEST)
        squared = jnp.maximum(row_norms[:, None] + norms[None, :] - 2.0 * crossed, 0.0)
        radius = jnp.sqrt(5.0 * squared)
        factor = factors[:, task_ids]
        shaped = (1.0 + radius + radius * radius / 3.0) * jnp.exp(-radius)
        kernel = (factor * shaped).astype(jnp.bfloat16)
        kernel_wide = lax.optimization_barrier(kernel).astype(jnp.float32)
        return jnp.dot(kernel_wide, rhs_wide, precision=lax.Precision.HIGHEST)
    starts = jnp.arange(4 * N_BLK, dtype=jnp.int32) * row_step
    blocks = lax.map(one_block, starts)
    return blocks.reshape(POINTS, RHS) + noise[0] * rhs_wide
```

```python
import math

import jax
import jax.numpy as jnp
from jax import lax
from jax.experimental import pallas as pl
from jax.experimental.pallas import tpu as pltpu
from jax.sharding import Mesh
from jax.sharding import PartitionSpec as P

FINE = ("zh", "zl", "xl", "core", "xh", "y")
COLS = ("zl", "xh", "xl")
FAR = "zh"
NEAR = ("y", "core")

LANES = 128
ONES = 96
NORMS = 99
TASK = 102

LN2 = math.log(2.0)
SCALE = 5.0 / (LN2 * LN2)
SHIFT = 1.5 / LN2
REST = 0.75 / (LN2 * LN2)
GAIN = LN2 * LN2 / 3.0 * math.exp(1.5)

ROW_STEP = 640
COL_STEP = 256


def split3(value):
    first = value.astype(jnp.bfloat16).astype(jnp.float32)
    left = value - first
    second = left.astype(jnp.bfloat16).astype(jnp.float32)
    third = (left - second).astype(jnp.bfloat16).astype(jnp.float32)
    return first, second, third


def pack_kernel(points, rhs, tasks, scales, rows_out, cols_out):
    count = points.shape[0]
    scaled = (points[...].astype(jnp.float32) / scales[...]).astype(jnp.bfloat16)
    wide = scaled.astype(jnp.float32)
    norms = jnp.sum(wide * wide, axis=1, keepdims=True) * SCALE
    pieces = split3(norms)
    labels = tasks[...].astype(jnp.float32)
    lane = lax.broadcasted_iota(jnp.int32, (count, 32), 1) + 96
    tail_rows = jnp.where(lane < NORMS, 1.0, 0.0)
    tail_cols = jnp.where((lane >= NORMS) & (lane < TASK), 1.0, 0.0)
    for index, piece in enumerate(pieces):
        tail_rows = jnp.where(lane == NORMS + index, piece, tail_rows)
        tail_cols = jnp.where(lane == ONES + index, piece, tail_cols)
    tail_rows = jnp.where(lane == TASK, labels, tail_rows)
    tail_cols = jnp.where(lane == TASK, labels, tail_cols)
    wide_rhs = rhs[...].astype(jnp.float32)
    rows = jnp.concatenate([wide, wide_rhs, tail_rows], axis=1).astype(jnp.bfloat16)
    cols = jnp.concatenate([wide, jnp.zeros_like(wide_rhs), tail_cols], axis=1).astype(jnp.bfloat16)
    for index in range(rows_out.shape[0]):
        rows_out[index] = rows
    for index in range(cols_out.shape[0]):
        cols_out[index] = cols


def pack(points, rhs, task_ids, length_scales, n_rows, n_cols):
    count = points.shape[0]
    return pl.pallas_call(
        pack_kernel,
        out_shape=(
            jax.ShapeDtypeStruct((n_rows, count, LANES), jnp.bfloat16),
            jax.ShapeDtypeStruct((n_cols, count, LANES), jnp.bfloat16),
        ),
        name="pack",
    )(points, rhs, task_ids[:, None], length_scales[None, :])


def shaped(scaled_squared):
    held = jnp.maximum(scaled_squared, 1e-30)
    root = held * lax.rsqrt(held)
    arg = -SHIFT - root
    return ((arg * arg + REST) * jnp.exp2(arg)).astype(jnp.bfloat16)


def tile_kernel(rows, cols, coregion, out, weights, spread, sums, dist_a, dist_b, ker_a, ker_b):
    n_rows, n_cols = rows.shape[0], cols.shape[0]
    n_tasks = coregion.shape[0]
    n_rhs = LANES // n_tasks
    row_blocks, col_blocks = n_rows // ROW_STEP, n_cols // COL_STEP
    steps = row_blocks * col_blocks

    lane = lax.broadcasted_iota(jnp.int32, (1, LANES), 1)
    gains = jnp.where(lane < 64, -2.0 * SCALE, jnp.where((lane >= ONES) & (lane < TASK), 1.0, 0.0))

    def build_weights(index, carry):
        at = pl.multiple_of(index * COL_STEP, COL_STEP)
        value = cols[pl.ds(at, COL_STEP), :].astype(jnp.float32) * gains
        high = value.astype(jnp.bfloat16)
        low = (value - high.astype(jnp.float32)).astype(jnp.bfloat16)
        weights[pl.ds(at, COL_STEP), 0:LANES] = high
        weights[pl.ds(at, COL_STEP), LANES : 2 * LANES] = low
        return carry

    lax.fori_loop(0, col_blocks, build_weights, 0)

    def build_spread(index, carry):
        at = pl.multiple_of(index * LANES, LANES)
        turned = rows[pl.ds(at, LANES), :].astype(jnp.float32).T
        vectors = turned[64 : 64 + n_rhs, :]
        label = turned[TASK : TASK + 1, :]
        parts = [jnp.where(label == float(task), vectors, 0.0) for task in range(n_tasks)]
        spread[:, pl.ds(at, LANES)] = jnp.concatenate(parts, axis=0).astype(jnp.bfloat16)
        return carry

    lax.fori_loop(0, n_rows // LANES, build_spread, 0)

    def places(step):
        block = step // row_blocks
        row = pl.multiple_of((step - block * row_blocks) * ROW_STEP, ROW_STEP)
        return row, pl.multiple_of(block * COL_STEP, COL_STEP)

    def distances(step, dist):
        row, col = places(step)
        left = rows[pl.ds(row, ROW_STEP), :]
        dist[...] = lax.dot_general(
            jnp.concatenate([left, left], axis=1),
            weights[pl.ds(col, COL_STEP), :],
            (((1,), (1,)), ((), ())),
            preferred_element_type=jnp.float32,
        )

    def values(dist, ker):
        ker[...] = shaped(dist[...])

    def product(step, ker):
        row, col = places(step)
        sums[:, pl.ds(col, COL_STEP)] += jnp.dot(
            spread[:, pl.ds(row, ROW_STEP)], ker[...], preferred_element_type=jnp.float32
        )

    sums[...] = jnp.zeros_like(sums)
    distances(0, dist_a)
    distances(1, dist_b)
    values(dist_a, ker_a)

    def pair(index, carry):
        step = index * 2
        distances(step, dist_a)
        values(dist_b, ker_b)
        product(step - 2, ker_a)
        distances(step + 1, dist_b)
        values(dist_a, ker_a)
        product(step - 1, ker_b)
        return carry

    lax.fori_loop(1, steps // 2, pair, 0)
    values(dist_b, ker_b)
    product(steps - 2, ker_a)
    product(steps - 1, ker_b)

    def finish(index, carry):
        at = pl.multiple_of(index * LANES, LANES)
        label = cols[pl.ds(at, LANES), :].astype(jnp.float32).T[TASK : TASK + 1, :]
        total = jnp.zeros((n_rhs, LANES), jnp.float32)
        for task in range(n_tasks):
            factor = jnp.zeros_like(label)
            for own in range(n_tasks):
                factor = jnp.where(label == float(own), coregion[own, task] * GAIN, factor)
            total = total + factor * sums[task * n_rhs : (task + 1) * n_rhs, pl.ds(at, LANES)]
        out[pl.ds(at, LANES), :] = total.T
        return carry

    lax.fori_loop(0, n_cols // LANES, finish, 0)


def tile(rows, cols, coregion):
    n_rows, n_cols = rows.shape[0], cols.shape[0]
    vmem = pl.BlockSpec(memory_space=pltpu.VMEM)
    return pl.pallas_call(
        tile_kernel,
        out_shape=jax.ShapeDtypeStruct((n_cols, LANES // coregion.shape[0]), jnp.float32),
        in_specs=[vmem, vmem, pl.BlockSpec(memory_space=pltpu.SMEM)],
        out_specs=vmem,
        scratch_shapes=[
            pltpu.VMEM((n_cols, 2 * LANES), jnp.bfloat16),
            pltpu.VMEM((LANES, n_rows), jnp.bfloat16),
            pltpu.VMEM((LANES, n_cols), jnp.float32),
            pltpu.VMEM((ROW_STEP, COL_STEP), jnp.float32),
            pltpu.VMEM((ROW_STEP, COL_STEP), jnp.float32),
            pltpu.VMEM((ROW_STEP, COL_STEP), jnp.bfloat16),
            pltpu.VMEM((ROW_STEP, COL_STEP), jnp.bfloat16),
        ],
        name="tile",
    )(rows, cols, coregion)


def exchange(blocks, axes):
    return lax.all_to_all(blocks, axes, 0, 0, tiled=True)


def body(points, task_ids, rhs, length_scales, coregion, noise):
    count, n_rhs = rhs.shape
    far, near, across = (lax.axis_size(axes) for axes in (FAR, NEAR, COLS))
    own_rows, own_cols = pack(points, rhs, task_ids, length_scales, far, across)
    rows = exchange(own_rows, FAR).reshape(far * count, LANES)
    cols = exchange(own_cols, COLS).reshape(across * count, LANES)
    rows = exchange(jnp.broadcast_to(rows, (near,) + rows.shape), NEAR).reshape(-1, LANES)
    partial = tile(rows, cols, coregion)
    back = exchange(partial.reshape(across, count, n_rhs), COLS)
    return jnp.sum(back, axis=0) + noise[0] * rhs.astype(jnp.float32)


def solution(mesh):
    finer = Mesh(mesh.devices.reshape(4, 4, 2, 2, 2, 4), FINE)
    placed = (P(FINE, None), P(FINE), P(FINE, None), P(), P(), P())
    return jax.shard_map(
        body, mesh=finer, in_specs=placed, out_specs=P(FINE, None), check_vma=False
    )
```

```python
import math

import jax
import jax.numpy as jnp
from jax import lax
from jax.experimental import pallas as pl
from jax.experimental.pallas import tpu as pltpu
from jax.sharding import Mesh
from jax.sharding import PartitionSpec as P

FINE = ("zh", "zl", "xl", "core", "xh", "y")
COLS = ("zl", "xh", "xl")
FAR = "zh"

LANES = 128
ONES = 96
NORMS = 99
TASK = 102
GROUPS = 4

LN2 = math.log(2.0)
SCALE = 5.0 / (LN2 * LN2)
SHIFT = 1.5 / LN2
REST = 0.75 / (LN2 * LN2)
GAIN = LN2 * LN2 / 3.0 * math.exp(1.5)

ROW_STEP = 5120
COL_STEP = 256

VMEM = pl.BlockSpec(memory_space=pltpu.VMEM)
SMEM = pl.BlockSpec(memory_space=pltpu.SMEM)


def split3(value):
    first = value.astype(jnp.bfloat16).astype(jnp.float32)
    left = value - first
    second = left.astype(jnp.bfloat16).astype(jnp.float32)
    third = (left - second).astype(jnp.bfloat16).astype(jnp.float32)
    return first, second, third


def pack_kernel(at_ref, points, rhs, tasks, scales, rows_out, cols_out):
    count = points.shape[1]
    quarter = count // GROUPS
    wide = (points[...].astype(jnp.float32) / scales[...]).astype(jnp.bfloat16).astype(jnp.float32)
    norms = jnp.sum(wide * wide, axis=0, keepdims=True) * SCALE
    labels = tasks[...].astype(jnp.float32)
    place = lax.broadcasted_iota(jnp.int32, (32, count), 0) + ONES
    tail = jnp.where(place < NORMS, 1.0, 0.0)
    for index, piece in enumerate(split3(norms)):
        tail = jnp.where(place == NORMS + index, piece, tail)
    tail = jnp.where(place == TASK, labels, tail)
    turned = jnp.concatenate([wide, rhs[...].astype(jnp.float32), tail], axis=0).T
    rows = turned.astype(jnp.bfloat16)
    for index in range(rows_out.shape[0]):
        rows_out[index] = rows
    half = count // 2
    features = turned[:, 0:64]
    paired = jnp.concatenate([features[0:half], features[half:count]], axis=1)
    start = lax.rem(at_ref[0] * quarter, LANES)
    lane = lax.broadcasted_iota(jnp.int32, (quarter, 2 * LANES), 1)
    point = lax.broadcasted_iota(jnp.int32, (quarter, 2 * LANES), 0)
    column = turned[:, TASK : TASK + 1]
    lines = []
    for group in range(GROUPS):
        own = column[group * quarter : (group + 1) * quarter]
        line = jnp.sum(jnp.where(lane == point + start, own, 0.0), axis=0, keepdims=True)
        lines += [line[:, 0:LANES], line[:, LANES : 2 * LANES]]
    cols = jnp.concatenate([paired] + lines, axis=0).astype(jnp.bfloat16)
    for index in range(cols_out.shape[0]):
        cols_out[index] = cols


def pack(at, points, rhs, task_ids, length_scales, n_rows, n_cols):
    count = points.shape[1]
    return pl.pallas_call(
        pack_kernel,
        out_shape=(
            jax.ShapeDtypeStruct((n_rows, count, LANES), jnp.bfloat16),
            jax.ShapeDtypeStruct((n_cols, count // 2 + 2 * GROUPS, LANES), jnp.bfloat16),
        ),
        in_specs=[SMEM, VMEM, VMEM, VMEM, VMEM],
        out_specs=(VMEM, VMEM),
        name="pack",
    )(at, points, rhs, task_ids[None, :], length_scales[:, None])


def weigh_kernel(cols, coregion, weights, factors, held, labels):
    pieces = cols.shape[0]
    half = cols.shape[1] - 2 * GROUPS
    quarter = half // 2
    wide = pieces * quarter
    for part in range(2):
        for piece in range(pieces):
            held[part * wide + piece * quarter : part * wide + (piece + 1) * quarter] = cols[
                piece, part * quarter : (part + 1) * quarter
            ].astype(jnp.float32)
    labels[...] = jnp.zeros_like(labels)
    for piece in range(pieces):
        lines = cols[piece, half : half + 2 * GROUPS].astype(jnp.float32)
        tile, spill = divmod(piece * quarter, LANES)
        for group in range(GROUPS):
            at = group * wide + tile * LANES
            labels[:, at : at + LANES] += lines[2 * group : 2 * group + 1]
            if spill + quarter > LANES:
                labels[:, at + LANES : at + 2 * LANES] += lines[2 * group + 1 : 2 * group + 2]
    for task in range(factors.shape[0]):
        factor = jnp.zeros_like(labels)
        for own in range(coregion.shape[0]):
            factor = jnp.where(labels[...] == float(own), coregion[own, task] * GAIN, factor)
        factors[task : task + 1] = factor
    for part in range(2):
        both = held[part * wide : (part + 1) * wide].T
        for side in range(2):
            at = (2 * side + part) * wide
            features = both[side * 64 : (side + 1) * 64]
            norms = jnp.sum(features * features, axis=0, keepdims=True) * SCALE
            value = features * (-2.0 * SCALE)
            high = value.astype(jnp.bfloat16)
            low = (value - high.astype(jnp.float32)).astype(jnp.bfloat16)
            place = lax.broadcasted_iota(jnp.int32, (32, wide), 0) + ONES
            tail = jnp.where((place >= NORMS) & (place < TASK), 1.0, 0.0)
            for index, piece in enumerate(split3(norms)):
                tail = jnp.where(place == ONES + index, piece, tail)
            blank = jnp.zeros((64, wide), jnp.bfloat16)
            weights[0:64, at : at + wide] = high
            weights[64:96, at : at + wide] = blank[0:32]
            weights[96:128, at : at + wide] = tail.astype(jnp.bfloat16)
            weights[128:192, at : at + wide] = low
            weights[192:256, at : at + wide] = blank


def weigh(cols, coregion):
    pieces, height, _ = cols.shape
    total = pieces * (height - 2 * GROUPS) * 2
    return pl.pallas_call(
        weigh_kernel,
        out_shape=(
            jax.ShapeDtypeStruct((2 * LANES, total), jnp.bfloat16),
            jax.ShapeDtypeStruct((coregion.shape[0], total), jnp.float32),
        ),
        in_specs=[VMEM, SMEM],
        out_specs=(VMEM, VMEM),
        scratch_shapes=[
            pltpu.VMEM((total // 2, LANES), jnp.float32),
            pltpu.VMEM((1, total), jnp.float32),
        ],
        name="weigh",
    )(cols, coregion)


def shaped(scaled_squared):
    held = jnp.maximum(scaled_squared, 1e-30)
    root = held * lax.rsqrt(held)
    arg = -SHIFT - root
    return ((arg * arg + REST) * jnp.exp2(arg)).astype(jnp.bfloat16)


def tile_kernel(rows, weights, factors, out, spread, sums, dist_a, dist_b, ker_a, ker_b):
    n_rows, n_cols = rows.shape[0], weights.shape[1]
    n_tasks = factors.shape[0]
    n_rhs = LANES // n_tasks
    row_blocks, col_blocks = n_rows // ROW_STEP, n_cols // COL_STEP
    steps = row_blocks * col_blocks

    def build_spread(index, carry):
        at = pl.multiple_of(index * ROW_STEP, ROW_STEP)
        turned = rows[pl.ds(at, ROW_STEP), :].astype(jnp.float32).T
        vectors = turned[64 : 64 + n_rhs, :]
        label = turned[TASK : TASK + 1, :]
        parts = [jnp.where(label == float(task), vectors, 0.0) for task in range(n_tasks)]
        spread[:, pl.ds(at, ROW_STEP)] = jnp.concatenate(parts, axis=0).astype(jnp.bfloat16)
        return carry

    lax.fori_loop(0, row_blocks, build_spread, 0)

    def places(step):
        block = step // row_blocks
        row = pl.multiple_of((step - block * row_blocks) * ROW_STEP, ROW_STEP)
        return row, pl.multiple_of(block * COL_STEP, COL_STEP)

    sums[...] = jnp.zeros_like(sums)

    def group(index, carry):
        for sub in range(1):
            step = index * 1 + sub
            row, col = places(step)
            left = rows[pl.ds(row, ROW_STEP), :]
            found = jnp.dot(
                jnp.concatenate([left, left], axis=1),
                weights[:, pl.ds(col, COL_STEP)],
                preferred_element_type=jnp.float32,
            )
            sums[:, pl.ds(col, COL_STEP)] += jnp.dot(
                spread[:, pl.ds(row, ROW_STEP)], shaped(found), preferred_element_type=jnp.float32
            )
        return carry

    lax.fori_loop(0, steps // 1, group, 0)
    wide = n_cols // GROUPS
    stacked = []
    for group in range(GROUPS):
        at = group * wide
        total = jnp.zeros((n_rhs, wide), jnp.float32)
        for task in range(n_tasks):
            total = total + (
                factors[task : task + 1, at : at + wide]
                * sums[task * n_rhs : (task + 1) * n_rhs, at : at + wide]
            )
        stacked.append(total)
    out[...] = jnp.concatenate(stacked, axis=0).T


def tile(rows, weights, factors):
    n_rows, n_cols = rows.shape[0], weights.shape[1]
    return pl.pallas_call(
        tile_kernel,
        out_shape=jax.ShapeDtypeStruct((n_cols // GROUPS, LANES), jnp.float32),
        in_specs=[VMEM, VMEM, VMEM],
        out_specs=VMEM,
        scratch_shapes=[
            pltpu.VMEM((LANES, n_rows), jnp.bfloat16),
            pltpu.VMEM((LANES, n_cols), jnp.float32),
            pltpu.VMEM((ROW_STEP, COL_STEP), jnp.float32),
            pltpu.VMEM((ROW_STEP, COL_STEP), jnp.float32),
            pltpu.VMEM((ROW_STEP, COL_STEP), jnp.bfloat16),
            pltpu.VMEM((ROW_STEP, COL_STEP), jnp.bfloat16),
        ],
        name="tile",
    )(rows, weights, factors)


def finish_kernel(parts, rhs, noise, out):
    total = jnp.sum(parts[...], axis=0).T
    n_rhs, _ = rhs.shape
    groups = [total[index * n_rhs : (index + 1) * n_rhs] for index in range(GROUPS)]
    out[...] = jnp.concatenate(groups, axis=1) + noise[0] * rhs[...].astype(jnp.float32)


def finish(parts, rhs, noise):
    return pl.pallas_call(
        finish_kernel,
        out_shape=jax.ShapeDtypeStruct(rhs.shape, jnp.float32),
        in_specs=[VMEM, VMEM, SMEM],
        out_specs=VMEM,
        name="finish",
    )(parts, rhs, noise)


def exchange(blocks, axes):
    return lax.all_to_all(blocks, axes, 0, 0, tiled=True)


def from_all(block, axes):
    return exchange(jnp.broadcast_to(block, (lax.axis_size(axes),) + block.shape), axes)


def body(points, task_ids, rhs, length_scales, coregion, noise):
    far, across = (lax.axis_size(axes) for axes in (FAR, COLS))
    at = lax.axis_index(COLS)[None].astype(jnp.int32)
    own_rows, own_cols = pack(at, points.T, rhs.T, task_ids, length_scales, far, across)
    rows = exchange(own_rows, FAR).reshape(-1, LANES)
    cols = exchange(own_cols, COLS)
    weights, factors = weigh(cols, coregion)
    rows = from_all(rows, "y").reshape(-1, LANES)
    rows = from_all(rows, "core").reshape(-1, LANES)
    partial = tile(rows, weights, factors)
    back = exchange(partial.reshape(across, -1, LANES), COLS)
    return finish(back, rhs.T, noise).T


def solution(mesh):
    finer = Mesh(mesh.devices.reshape(4, 4, 2, 2, 2, 4), FINE)
    placed = (P(FINE, None), P(FINE), P(FINE, None), P(), P(), P())
    return jax.shard_map(
        body, mesh=finer, in_specs=placed, out_specs=P(FINE, None), check_vma=False
    )
```

```python
import functools
import math

import jax
import jax.numpy as jnp
from jax import lax
from jax.experimental import pallas as pl
from jax.experimental.pallas import tpu as pltpu
from jax.sharding import Mesh
from jax.sharding import PartitionSpec as P

FINE = ("zh", "zl", "xl", "core", "xh", "y")
COLS = ("xh", "xl", "y")
FAR = "zh"
NEAR = "zl"

LANES = 128
ONES = 96
NORMS = 99
TASK = 102
GROUPS = 4

LN2 = math.log(2.0)
SCALE = 5.0 / (LN2 * LN2)
SHIFT = 1.5 / LN2
REST = 0.75 / (LN2 * LN2)
GAIN = LN2 * LN2 / 3.0 * math.exp(1.5)

COL_STEP = 256


VMEM = pl.BlockSpec(memory_space=pltpu.VMEM)
SMEM = pl.BlockSpec(memory_space=pltpu.SMEM)


def split3(value):
    first = value.astype(jnp.bfloat16).astype(jnp.float32)
    left = value - first
    second = left.astype(jnp.bfloat16).astype(jnp.float32)
    third = (left - second).astype(jnp.bfloat16).astype(jnp.float32)
    return first, second, third


def pack_kernel(at_ref, points, rhs, tasks, scales, rows_out, cols_out):
    count = points.shape[1]
    quarter = count // GROUPS
    column = jnp.broadcast_to(scales[...], (8, scales.shape[1])).T[:, 0:1]
    wide = (points[...].astype(jnp.float32) / column).astype(jnp.bfloat16).astype(jnp.float32)
    norms = jnp.sum(wide * wide, axis=0, keepdims=True) * SCALE
    labels = tasks[...].astype(jnp.float32)
    place = lax.broadcasted_iota(jnp.int32, (32, count), 0) + ONES
    tail = jnp.where(place < NORMS, 1.0, 0.0)
    for index, piece in enumerate(split3(norms)):
        tail = jnp.where(place == NORMS + index, piece, tail)
    tail = jnp.where(place == TASK, labels, tail)
    turned = jnp.concatenate([wide, rhs[...].astype(jnp.float32), tail], axis=0).T
    rows = turned.astype(jnp.bfloat16)
    rows_out[...] = rows
    half = count // 2
    features = turned[:, 0:64]
    paired = jnp.concatenate([features[0:half], features[half:count]], axis=1)
    start = lax.rem(at_ref[0] * quarter, LANES)
    lane = lax.broadcasted_iota(jnp.int32, (quarter, 2 * LANES), 1)
    point = lax.broadcasted_iota(jnp.int32, (quarter, 2 * LANES), 0)
    column = turned[:, TASK : TASK + 1]
    lines = []
    for group in range(GROUPS):
        own = column[group * quarter : (group + 1) * quarter]
        line = jnp.sum(jnp.where(lane == point + start, own, 0.0), axis=0, keepdims=True)
        lines += [line[:, 0:LANES], line[:, LANES : 2 * LANES]]
    cols = jnp.concatenate([paired] + lines, axis=0).astype(jnp.bfloat16)
    for index in range(cols_out.shape[0]):
        cols_out[index] = cols


def pack(at, points, rhs, task_ids, length_scales, n_cols):
    count = points.shape[1]
    return pl.pallas_call(
        pack_kernel,
        out_shape=(
            jax.ShapeDtypeStruct((count, LANES), jnp.bfloat16),
            jax.ShapeDtypeStruct((n_cols, count // 2 + 2 * GROUPS, LANES), jnp.bfloat16),
        ),
        in_specs=[SMEM, VMEM, VMEM, VMEM, VMEM],
        out_specs=(VMEM, VMEM),
        name="pack",
    )(at, points, rhs, task_ids[None, :], length_scales[None, :])


def weigh_kernel(cols, coregion, weights, factors, held, labels):
    pieces = cols.shape[0]
    half = cols.shape[1] - 2 * GROUPS
    quarter = half // 2
    wide = pieces * quarter
    for part in range(2):
        for piece in range(pieces):
            held[part * wide + piece * quarter : part * wide + (piece + 1) * quarter] = cols[
                piece, part * quarter : (part + 1) * quarter
            ].astype(jnp.float32)
    labels[...] = jnp.zeros_like(labels)
    for piece in range(pieces):
        lines = cols[piece, half : half + 2 * GROUPS].astype(jnp.float32)
        tile, spill = divmod(piece * quarter, LANES)
        for group in range(GROUPS):
            at = group * wide + tile * LANES
            labels[:, at : at + LANES] += lines[2 * group : 2 * group + 1]
            if spill + quarter > LANES:
                labels[:, at + LANES : at + 2 * LANES] += lines[2 * group + 1 : 2 * group + 2]
    for task in range(factors.shape[0]):
        factor = jnp.zeros_like(labels)
        for own in range(coregion.shape[0]):
            factor = jnp.where(labels[...] == float(own), coregion[own, task] * GAIN, factor)
        factors[task : task + 1] = factor
    for part in range(2):
        both = held[part * wide : (part + 1) * wide].T
        for side in range(2):
            at = (2 * side + part) * wide
            features = both[side * 64 : (side + 1) * 64]
            norms = jnp.sum(features * features, axis=0, keepdims=True) * SCALE
            value = features * (-2.0 * SCALE)
            high = value.astype(jnp.bfloat16)
            low = (value - high.astype(jnp.float32)).astype(jnp.bfloat16)
            place = lax.broadcasted_iota(jnp.int32, (32, wide), 0) + ONES
            tail = jnp.where((place >= NORMS) & (place < TASK), 1.0, 0.0)
            for index, piece in enumerate(split3(norms)):
                tail = jnp.where(place == ONES + index, piece, tail)
            blank = jnp.zeros((64, wide), jnp.bfloat16)
            weights[0:64, at : at + wide] = high
            weights[64:96, at : at + wide] = blank[0:32]
            weights[96:128, at : at + wide] = tail.astype(jnp.bfloat16)
            weights[128:192, at : at + wide] = low
            weights[192:256, at : at + wide] = blank


def weigh(cols, coregion):
    pieces, height, _ = cols.shape
    total = pieces * (height - 2 * GROUPS) * 2
    return pl.pallas_call(
        weigh_kernel,
        out_shape=(
            jax.ShapeDtypeStruct((2 * LANES, total), jnp.bfloat16),
            jax.ShapeDtypeStruct((coregion.shape[0], total), jnp.float32),
        ),
        in_specs=[VMEM, SMEM],
        out_specs=(VMEM, VMEM),
        scratch_shapes=[
            pltpu.VMEM((total // 2, LANES), jnp.float32),
            pltpu.VMEM((1, total), jnp.float32),
        ],
        name="weigh",
    )(cols, coregion)


def shaped(scaled_squared):
    held = jnp.maximum(scaled_squared, 1e-30)
    root = held * lax.rsqrt(held)
    arg = -SHIFT - root
    return ((arg * arg + REST) * jnp.exp2(arg)).astype(jnp.bfloat16)


def tile_kernel(n_sources, skip_own, unroll, own, *refs):
    sources, (weights, factors, given, out, held, spread, sums) = refs[:n_sources], refs[n_sources:]
    n_cols = weights.shape[1]
    n_tasks = factors.shape[0]
    n_rhs = LANES // n_tasks

    at = 0
    for source in sources:
        blocks, count, _ = source.shape
        for index in range(1, blocks) if skip_own else range(blocks):
            place = lax.rem(own[0] + index, blocks) if skip_own else index
            held[at : at + count] = source[place]
            at += count

    turned = held[...].astype(jnp.float32).T
    vectors = turned[64 : 64 + n_rhs, :]
    label = turned[TASK : TASK + 1, :]
    parts = [jnp.where(label == float(task), vectors, 0.0) for task in range(n_tasks)]
    spread[...] = jnp.concatenate(parts, axis=0).astype(jnp.bfloat16)

    def group(index, carry):
        for sub in range(unroll):
            col = pl.multiple_of((index * unroll + sub) * COL_STEP, COL_STEP)
            left = held[...]
            found = jnp.dot(
                jnp.concatenate([left, left], axis=1),
                weights[:, pl.ds(col, COL_STEP)],
                preferred_element_type=jnp.float32,
            )
            sums[:, pl.ds(col, COL_STEP)] = jnp.dot(
                spread[...], shaped(found), preferred_element_type=jnp.float32
            )
        return carry

    lax.fori_loop(0, n_cols // COL_STEP // unroll, group, 0)

    wide = n_cols // GROUPS
    stacked = []
    for index in range(GROUPS):
        at = index * wide
        total = jnp.zeros((n_rhs, wide), jnp.float32)
        for task in range(n_tasks):
            total = total + (
                factors[task : task + 1, at : at + wide]
                * sums[task * n_rhs : (task + 1) * n_rhs, at : at + wide]
            )
        stacked.append(total)
    out[...] = jnp.concatenate(stacked, axis=0).T + given[...]


def tile(sources, own, weights, factors, given, skip_own, unroll):
    n_cols = weights.shape[1]
    n_rows = sum((s.shape[0] - (1 if skip_own else 0)) * s.shape[1] for s in sources)
    return pl.pallas_call(
        functools.partial(tile_kernel, len(sources), skip_own, unroll),
        out_shape=jax.ShapeDtypeStruct((n_cols // GROUPS, LANES), jnp.float32),
        in_specs=[SMEM] + [VMEM] * (len(sources) + 3),
        out_specs=VMEM,
        scratch_shapes=[
            pltpu.VMEM((n_rows, LANES), jnp.bfloat16),
            pltpu.VMEM((LANES, n_rows), jnp.bfloat16),
            pltpu.VMEM((LANES, n_cols), jnp.float32),
        ],
    )(own, *sources, weights, factors, given)


def finish_kernel(parts, rhs, noise, out):
    total = jnp.sum(parts[...], axis=0).T
    n_rhs, _ = rhs.shape
    groups = [total[index * n_rhs : (index + 1) * n_rhs] for index in range(GROUPS)]
    out[...] = jnp.concatenate(groups, axis=1) + noise[0] * rhs[...].astype(jnp.float32)


def finish(parts, rhs, noise):
    return pl.pallas_call(
        finish_kernel,
        out_shape=jax.ShapeDtypeStruct(rhs.shape, jnp.float32),
        in_specs=[VMEM, VMEM, SMEM],
        out_specs=VMEM,
        name="finish",
    )(parts, rhs, noise)


def exchange(blocks, axes):
    return lax.all_to_all(blocks, axes, 0, 0, tiled=True)


def from_shift(value, axis, shift):
    count = lax.axis_size(axis)
    return lax.ppermute(value, axis, [(i, (i + shift) % count) for i in range(count)])


def body(points, task_ids, rhs, length_scales, coregion, noise):
    far, near, across = (lax.axis_size(axes) for axes in (FAR, NEAR, COLS))
    at = lax.axis_index(COLS)[None].astype(jnp.int32)
    own = lax.axis_index(NEAR)[None].astype(jnp.int32)
    own_rows, own_cols = pack(at, points.T, rhs.T, task_ids, length_scales, across)
    others = [from_shift(own_rows, FAR, shift) for shift in (far // 2, 1, far - 1)]
    cols = exchange(own_cols, COLS)
    rows = jnp.stack([own_rows] + others)
    twin = from_shift(rows, "core", 1)
    rows = rows.reshape(1, -1, LANES)
    all_rows = exchange(jnp.broadcast_to(rows, (near,) + rows.shape[1:]), NEAR)
    weights, factors = weigh(cols, coregion)
    empty = jnp.zeros((weights.shape[1] // GROUPS, LANES), jnp.float32)
    first = (rows, twin.reshape(rows.shape))
    total = tile(first, own, weights, factors, empty, False, 5)
    twins = from_shift(all_rows, "core", 1)
    total = tile((all_rows,), own, weights, factors, total, True, 2)
    total = tile((twins,), own, weights, factors, total, True, 2)
    back = exchange(total.reshape(across, -1, LANES), COLS)
    return finish(back, rhs.T, noise).T


def solution(mesh):
    finer = Mesh(mesh.devices.reshape(4, 4, 2, 2, 2, 4), FINE)
    placed = (P(FINE, None), P(FINE), P(FINE, None), P(), P(), P())
    return jax.shard_map(
        body, mesh=finer, in_specs=placed, out_specs=P(FINE, None), check_vma=False
    )
```

```python
import functools
import math

import jax
import jax.numpy as jnp
from jax import lax
from jax.experimental import pallas as pl
from jax.experimental.pallas import tpu as pltpu
from jax.sharding import Mesh
from jax.sharding import PartitionSpec as P

FINE = ("zh", "zl", "xl", "core", "xh", "y")
COLS = ("zl", "xh", "xl")
FAR = "zh"
NEAR = "y"

LANES = 128
ONES = 96
NORMS = 99
TASK = 102
GROUPS = 4

LN2 = math.log(2.0)
SCALE = 5.0 / (LN2 * LN2)
SHIFT = 1.5 / LN2
REST = 0.75 / (LN2 * LN2)
GAIN = LN2 * LN2 / 3.0 * math.exp(1.5)

COL_STEP = 256


VMEM = pl.BlockSpec(memory_space=pltpu.VMEM)
SMEM = pl.BlockSpec(memory_space=pltpu.SMEM)


def hold(value):
    return pltpu.with_memory_space_constraint(value, pltpu.VMEM)


def split3(value):
    first = value.astype(jnp.bfloat16).astype(jnp.float32)
    left = value - first
    second = left.astype(jnp.bfloat16).astype(jnp.float32)
    third = (left - second).astype(jnp.bfloat16).astype(jnp.float32)
    return first, second, third


def pack_kernel(at_ref, points, rhs, tasks, scales, rows_out, cols_out):
    count = points.shape[1]
    quarter = count // GROUPS
    column = jnp.broadcast_to(scales[...], (8, scales.shape[1])).T[:, 0:1]
    wide = (points[...].astype(jnp.float32) / column).astype(jnp.bfloat16).astype(jnp.float32)
    norms = jnp.sum(wide * wide, axis=0, keepdims=True) * SCALE
    labels = tasks[...].astype(jnp.float32)
    place = lax.broadcasted_iota(jnp.int32, (32, count), 0) + ONES
    tail = jnp.where(place < NORMS, 1.0, 0.0)
    for index, piece in enumerate(split3(norms)):
        tail = jnp.where(place == NORMS + index, piece, tail)
    tail = jnp.where(place == TASK, labels, tail)
    turned = jnp.concatenate([wide, rhs[...].astype(jnp.float32), tail], axis=0).T
    rows = turned.astype(jnp.bfloat16)
    rows_out[...] = rows
    half = count // 2
    features = turned[:, 0:64]
    paired = jnp.concatenate([features[0:half], features[half:count]], axis=1)
    start = lax.rem(at_ref[0] * quarter, LANES)
    lane = lax.broadcasted_iota(jnp.int32, (quarter, 2 * LANES), 1)
    point = lax.broadcasted_iota(jnp.int32, (quarter, 2 * LANES), 0)
    column = turned[:, TASK : TASK + 1]
    lines = []
    for group in range(GROUPS):
        own = column[group * quarter : (group + 1) * quarter]
        line = jnp.sum(jnp.where(lane == point + start, own, 0.0), axis=0, keepdims=True)
        lines += [line[:, 0:LANES], line[:, LANES : 2 * LANES]]
    cols = jnp.concatenate([paired] + lines, axis=0).astype(jnp.bfloat16)
    for index in range(cols_out.shape[0]):
        cols_out[index] = cols


def pack(at, points, rhs, task_ids, length_scales, n_cols):
    count = points.shape[1]
    return pl.pallas_call(
        pack_kernel,
        out_shape=(
            pltpu.VMEM((count, LANES), jnp.bfloat16),
            pltpu.VMEM((n_cols, count // 2 + 2 * GROUPS, LANES), jnp.bfloat16),
        ),
        in_specs=[SMEM, VMEM, VMEM, VMEM, VMEM],
        out_specs=(VMEM, VMEM),
        name="pack",
    )(at, points, rhs, task_ids[None, :], length_scales[None, :])


def weigh_kernel(cols, coregion, weights, factors, held, labels):
    pieces = cols.shape[0]
    half = cols.shape[1] - 2 * GROUPS
    quarter = half // 2
    wide = pieces * quarter
    for part in range(2):
        for piece in range(pieces):
            held[part * wide + piece * quarter : part * wide + (piece + 1) * quarter] = cols[
                piece, part * quarter : (part + 1) * quarter
            ].astype(jnp.float32)
    labels[...] = jnp.zeros_like(labels)
    for piece in range(pieces):
        lines = cols[piece, half : half + 2 * GROUPS].astype(jnp.float32)
        tile, spill = divmod(piece * quarter, LANES)
        for group in range(GROUPS):
            at = group * wide + tile * LANES
            labels[:, at : at + LANES] += lines[2 * group : 2 * group + 1]
            if spill + quarter > LANES:
                labels[:, at + LANES : at + 2 * LANES] += lines[2 * group + 1 : 2 * group + 2]
    for task in range(factors.shape[0]):
        factor = jnp.zeros_like(labels)
        for own in range(coregion.shape[0]):
            factor = jnp.where(labels[...] == float(own), coregion[own, task] * GAIN, factor)
        factors[task : task + 1] = factor
    for part in range(2):
        both = held[part * wide : (part + 1) * wide].T
        for side in range(2):
            at = (2 * side + part) * wide
            features = both[side * 64 : (side + 1) * 64]
            norms = jnp.sum(features * features, axis=0, keepdims=True) * SCALE
            value = features * (-2.0 * SCALE)
            high = value.astype(jnp.bfloat16)
            low = (value - high.astype(jnp.float32)).astype(jnp.bfloat16)
            place = lax.broadcasted_iota(jnp.int32, (32, wide), 0) + ONES
            tail = jnp.where((place >= NORMS) & (place < TASK), 1.0, 0.0)
            for index, piece in enumerate(split3(norms)):
                tail = jnp.where(place == ONES + index, piece, tail)
            blank = jnp.zeros((64, wide), jnp.bfloat16)
            weights[0:64, at : at + wide] = high
            weights[64:96, at : at + wide] = blank[0:32]
            weights[96:128, at : at + wide] = tail.astype(jnp.bfloat16)
            weights[128:192, at : at + wide] = low
            weights[192:256, at : at + wide] = blank


def weigh(cols, coregion):
    pieces, height, _ = cols.shape
    total = pieces * (height - 2 * GROUPS) * 2
    return pl.pallas_call(
        weigh_kernel,
        out_shape=(
            pltpu.VMEM((2 * LANES, total), jnp.bfloat16),
            pltpu.VMEM((coregion.shape[0], total), jnp.float32),
        ),
        in_specs=[VMEM, SMEM],
        out_specs=(VMEM, VMEM),
        scratch_shapes=[
            pltpu.VMEM((total // 2, LANES), jnp.float32),
            pltpu.VMEM((1, total), jnp.float32),
        ],
        name="weigh",
    )(hold(cols), coregion)


def shaped(scaled_squared):
    held = jnp.maximum(scaled_squared, 1e-30)
    root = held * lax.rsqrt(held)
    arg = -SHIFT - root
    return ((arg * arg + REST) * jnp.exp2(arg)).astype(jnp.bfloat16)


def tile_kernel(n_sources, skip_own, unroll, own, *refs):
    sources, (weights, factors), given = refs[:n_sources], refs[n_sources : n_sources + 2], refs[n_sources + 2 : -4]
    out, held, spread, sums = refs[-4:]
    n_cols = weights.shape[1]
    n_tasks = factors.shape[0]
    n_rhs = LANES // n_tasks

    at = 0
    for source in sources:
        blocks, count, _ = source.shape
        for index in range(1, blocks) if skip_own else range(blocks):
            place = lax.rem(own[0] + index, blocks) if skip_own else index
            held[at : at + count] = source[place]
            at += count

    turned = held[...].astype(jnp.float32).T
    vectors = turned[64 : 64 + n_rhs, :]
    label = turned[TASK : TASK + 1, :]
    parts = [jnp.where(label == float(task), vectors, 0.0) for task in range(n_tasks)]
    spread[...] = jnp.concatenate(parts, axis=0).astype(jnp.bfloat16)

    def group(index, carry):
        for sub in range(unroll):
            col = pl.multiple_of((index * unroll + sub) * COL_STEP, COL_STEP)
            left = held[...]
            found = jnp.dot(
                jnp.concatenate([left, left], axis=1),
                weights[:, pl.ds(col, COL_STEP)],
                preferred_element_type=jnp.float32,
            )
            sums[:, pl.ds(col, COL_STEP)] = jnp.dot(
                spread[...], shaped(found), preferred_element_type=jnp.float32
            )
        return carry

    lax.fori_loop(0, n_cols // COL_STEP // unroll, group, 0)

    wide = n_cols // GROUPS
    stacked = []
    for index in range(GROUPS):
        at = index * wide
        total = jnp.zeros((n_rhs, wide), jnp.float32)
        for task in range(n_tasks):
            total = total + (
                factors[task : task + 1, at : at + wide]
                * sums[task * n_rhs : (task + 1) * n_rhs, at : at + wide]
            )
        stacked.append(total)
    result = jnp.concatenate(stacked, axis=0).T
    for before in given:
        result = result + before[...]
    out[...] = result.astype(out.dtype)


def tile(sources, own, weights, factors, given, skip_own, unroll, out_dtype=jnp.float32):
    n_cols = weights.shape[1]
    n_rows = sum((s.shape[0] - (1 if skip_own else 0)) * s.shape[1] for s in sources)
    return pl.pallas_call(
        functools.partial(tile_kernel, len(sources), skip_own, unroll),
        out_shape=pltpu.VMEM((n_cols // GROUPS, LANES), out_dtype),
        in_specs=[SMEM] + [VMEM] * (len(sources) + 2 + len(given)),
        out_specs=VMEM,
        scratch_shapes=[
            pltpu.VMEM((n_rows, LANES), jnp.bfloat16),
            pltpu.VMEM((LANES, n_rows), jnp.bfloat16),
            pltpu.VMEM((LANES, n_cols), jnp.float32),
        ],
    )(own, *[hold(v) for v in sources], hold(weights), hold(factors), *[hold(v) for v in given])


def join_kernel(*refs):
    pieces, rows, copies = refs[:-2], refs[-2], refs[-1]
    for index, piece in enumerate(pieces):
        rows[index] = piece[...]
        count = piece.shape[0]
        for copy in range(copies.shape[0]):
            copies[copy, index * count : (index + 1) * count] = piece[...]


def join(pieces, n_copies):
    count = pieces[0].shape[0]
    return pl.pallas_call(
        join_kernel,
        out_shape=(
            pltpu.VMEM((len(pieces), count, LANES), jnp.bfloat16),
            pltpu.VMEM((n_copies, len(pieces) * count, LANES), jnp.bfloat16),
        ),
        in_specs=[VMEM] * len(pieces),
        out_specs=(VMEM, VMEM),
        name="join",
    )(*[hold(piece) for piece in pieces])


def finish_kernel(parts, rhs, noise, out):
    total = jnp.sum(parts[...].astype(jnp.float32), axis=0).T
    n_rhs, _ = rhs.shape
    groups = [total[index * n_rhs : (index + 1) * n_rhs] for index in range(GROUPS)]
    out[...] = jnp.concatenate(groups, axis=1) + noise[0] * rhs[...].astype(jnp.float32)


def finish(parts, rhs, noise):
    return pl.pallas_call(
        finish_kernel,
        out_shape=jax.ShapeDtypeStruct(rhs.shape, jnp.float32),
        in_specs=[VMEM, VMEM, SMEM],
        out_specs=VMEM,
        name="finish",
    )(hold(parts), rhs, noise)


def exchange(blocks, axes):
    return lax.all_to_all(blocks, axes, 0, 0, tiled=True)


def from_shift(value, axis, shift):
    count = lax.axis_size(axis)
    return lax.ppermute(value, axis, [(i, (i + shift) % count) for i in range(count)])


def body(points, task_ids, rhs, length_scales, coregion, noise):
    far, near, across = (lax.axis_size(axes) for axes in (FAR, NEAR, COLS))
    at = lax.axis_index(COLS)[None].astype(jnp.int32)
    own = lax.axis_index(NEAR)[None].astype(jnp.int32)
    own_rows, own_cols = pack(at, points.T, rhs.T, task_ids, length_scales, across)
    others = [from_shift(own_rows, FAR, shift) for shift in (far // 2, 1, far - 1)]
    cols = exchange(own_cols, COLS)
    rows, copies = join([own_rows] + others, near)
    twin = from_shift(rows, "core", 1)
    all_rows = exchange(copies, NEAR)
    weights, factors = weigh(cols, coregion)
    first = [value.reshape(1, -1, LANES) for value in (rows, twin)]
    total = tile(first, own, weights, factors, [], False, 10)
    twins = from_shift(all_rows, "core", 1)
    total = tile([all_rows], own, weights, factors, [total], True, 10)
    total = tile([twins], own, weights, factors, [total], True, 10, jnp.bfloat16)
    back = exchange(total.reshape(across, -1, LANES), COLS)
    return finish(back, rhs.T, noise).T


def solution(mesh):
    finer = Mesh(mesh.devices.reshape(4, 4, 2, 2, 2, 4), FINE)
    placed = (P(FINE, None), P(FINE), P(FINE, None), P(), P(), P())
    return jax.shard_map(
        body, mesh=finer, in_specs=placed, out_specs=P(FINE, None), check_vma=False
    )
```

```python
import functools
import math

import jax
import jax.numpy as jnp
from jax import lax
from jax.experimental import pallas as pl
from jax.experimental.pallas import tpu as pltpu
from jax.sharding import Mesh
from jax.sharding import PartitionSpec as P

FINE = ("zh", "zl", "xl", "core", "xh", "y")
COLS = ("zl", "xh", "xl")
FAR = "zh"
NEAR = "y"

LANES = 128
ONES = 96
NORMS = 99
TASK = 102
GROUPS = 4

LN2 = math.log(2.0)
SCALE = 5.0 / (LN2 * LN2)
SHIFT = 1.5 / LN2
REST = 0.75 / (LN2 * LN2)
GAIN = LN2 * LN2 / 3.0 * math.exp(1.5)

COL_STEP = 256


VMEM = pl.BlockSpec(memory_space=pltpu.VMEM)
ANY = pl.BlockSpec(memory_space=pl.ANY)
SMEM = pl.BlockSpec(memory_space=pltpu.SMEM)


def hold(value):
    return pltpu.with_memory_space_constraint(value, pltpu.VMEM)


def split3(value):
    first = value.astype(jnp.bfloat16).astype(jnp.float32)
    left = value - first
    second = left.astype(jnp.bfloat16).astype(jnp.float32)
    third = (left - second).astype(jnp.bfloat16).astype(jnp.float32)
    return first, second, third


def pack_kernel(at_ref, points, rhs, tasks, scales, rows_out, cols_out):
    count = points.shape[1]
    quarter = count // GROUPS
    column = jnp.broadcast_to(scales[...], (8, scales.shape[1])).T[:, 0:1]
    wide = (points[...].astype(jnp.float32) / column).astype(jnp.bfloat16).astype(jnp.float32)
    norms = jnp.sum(wide * wide, axis=0, keepdims=True) * SCALE
    labels = tasks[...].astype(jnp.float32)
    place = lax.broadcasted_iota(jnp.int32, (32, count), 0) + ONES
    tail = jnp.where(place < NORMS, 1.0, 0.0)
    for index, piece in enumerate(split3(norms)):
        tail = jnp.where(place == NORMS + index, piece, tail)
    tail = jnp.where(place == TASK, labels, tail)
    turned = jnp.concatenate([wide, rhs[...].astype(jnp.float32), tail], axis=0).T
    rows = turned.astype(jnp.bfloat16)
    rows_out[...] = rows
    half = count // 2
    features = turned[:, 0:64]
    paired = jnp.concatenate([features[0:half], features[half:count]], axis=1)
    start = lax.rem(at_ref[0] * quarter, LANES)
    lane = lax.broadcasted_iota(jnp.int32, (quarter, 2 * LANES), 1)
    point = lax.broadcasted_iota(jnp.int32, (quarter, 2 * LANES), 0)
    column = turned[:, TASK : TASK + 1]
    lines = []
    for group in range(GROUPS):
        own = column[group * quarter : (group + 1) * quarter]
        line = jnp.sum(jnp.where(lane == point + start, own, 0.0), axis=0, keepdims=True)
        lines += [line[:, 0:LANES], line[:, LANES : 2 * LANES]]
    cols = jnp.concatenate([paired] + lines, axis=0).astype(jnp.bfloat16)
    for index in range(cols_out.shape[0]):
        cols_out[index] = cols


def pack(at, points, rhs, task_ids, length_scales, n_cols):
    count = points.shape[1]
    return pl.pallas_call(
        pack_kernel,
        out_shape=(
            pltpu.VMEM((count, LANES), jnp.bfloat16),
            pltpu.VMEM((n_cols, count // 2 + 2 * GROUPS, LANES), jnp.bfloat16),
        ),
        in_specs=[SMEM, VMEM, VMEM, VMEM, VMEM],
        out_specs=(VMEM, VMEM),
        name="pack",
    )(at, points, rhs, task_ids[None, :], length_scales[None, :])


def weigh_kernel(cols, coregion, weights, factors, held, labels):
    pieces = cols.shape[0]
    half = cols.shape[1] - 2 * GROUPS
    quarter = half // 2
    wide = pieces * quarter
    for part in range(2):
        for piece in range(pieces):
            held[part * wide + piece * quarter : part * wide + (piece + 1) * quarter] = cols[
                piece, part * quarter : (part + 1) * quarter
            ].astype(jnp.float32)
    labels[...] = jnp.zeros_like(labels)
    for piece in range(pieces):
        lines = cols[piece, half : half + 2 * GROUPS].astype(jnp.float32)
        tile, spill = divmod(piece * quarter, LANES)
        for group in range(GROUPS):
            at = group * wide + tile * LANES
            labels[:, at : at + LANES] += lines[2 * group : 2 * group + 1]
            if spill + quarter > LANES:
                labels[:, at + LANES : at + 2 * LANES] += lines[2 * group + 1 : 2 * group + 2]
    for task in range(factors.shape[0]):
        factor = jnp.zeros_like(labels)
        for own in range(coregion.shape[0]):
            factor = jnp.where(labels[...] == float(own), coregion[own, task] * GAIN, factor)
        factors[task : task + 1] = factor
    for part in range(2):
        both = held[part * wide : (part + 1) * wide].T
        for side in range(2):
            at = (2 * side + part) * wide
            features = both[side * 64 : (side + 1) * 64]
            norms = jnp.sum(features * features, axis=0, keepdims=True) * SCALE
            value = features * (-2.0 * SCALE)
            high = value.astype(jnp.bfloat16)
            low = (value - high.astype(jnp.float32)).astype(jnp.bfloat16)
            place = lax.broadcasted_iota(jnp.int32, (32, wide), 0) + ONES
            tail = jnp.where((place >= NORMS) & (place < TASK), 1.0, 0.0)
            for index, piece in enumerate(split3(norms)):
                tail = jnp.where(place == ONES + index, piece, tail)
            blank = jnp.zeros((64, wide), jnp.bfloat16)
            weights[0:64, at : at + wide] = high
            weights[64:96, at : at + wide] = blank[0:32]
            weights[96:128, at : at + wide] = tail.astype(jnp.bfloat16)
            weights[128:192, at : at + wide] = low
            weights[192:256, at : at + wide] = blank


def weigh(cols, coregion):
    pieces, height, _ = cols.shape
    total = pieces * (height - 2 * GROUPS) * 2
    return pl.pallas_call(
        weigh_kernel,
        out_shape=(
            pltpu.VMEM((2 * LANES, total), jnp.bfloat16),
            pltpu.VMEM((coregion.shape[0], total), jnp.float32),
        ),
        in_specs=[VMEM, SMEM],
        out_specs=(VMEM, VMEM),
        scratch_shapes=[
            pltpu.VMEM((total // 2, LANES), jnp.float32),
            pltpu.VMEM((1, total), jnp.float32),
        ],
        name="weigh",
    )(hold(cols), coregion)


def shaped(scaled_squared):
    held = jnp.maximum(scaled_squared, 1e-30)
    root = held * lax.rsqrt(held)
    arg = -SHIFT - root
    return ((arg * arg + REST) * jnp.exp2(arg)).astype(jnp.bfloat16)


def tile_kernel(n_sources, skip_own, unroll, own, *refs):
    sources, (weights, factors), given = refs[:n_sources], refs[n_sources : n_sources + 2], refs[n_sources + 2 : -5]
    out, held, spread, sums, arrived = refs[-5:]
    n_cols = weights.shape[1]
    n_tasks = factors.shape[0]
    n_rhs = LANES // n_tasks

    at, copies = 0, []
    for source in sources:
        blocks, count, _ = source.shape
        for index in range(1, blocks) if skip_own else range(blocks):
            place = lax.rem(own[0] + index, blocks) if skip_own else index
            target = held.at[pl.ds(at, count)]
            copies.append(
                pltpu.make_async_copy(source.at[place], target, arrived.at[len(copies)])
            )
            at += count
    for copy in copies:
        copy.start()
    for copy in copies:
        copy.wait()

    turned = held[...].astype(jnp.float32).T
    vectors = turned[64 : 64 + n_rhs, :]
    label = turned[TASK : TASK + 1, :]
    parts = [jnp.where(label == float(task), vectors, 0.0) for task in range(n_tasks)]
    spread[...] = jnp.concatenate(parts, axis=0).astype(jnp.bfloat16)

    def group(index, carry):
        for sub in range(unroll):
            col = pl.multiple_of((index * unroll + sub) * COL_STEP, COL_STEP)
            left = held[...]
            found = jnp.dot(
                jnp.concatenate([left, left], axis=1),
                weights[:, pl.ds(col, COL_STEP)],
                preferred_element_type=jnp.float32,
            )
            sums[:, pl.ds(col, COL_STEP)] = jnp.dot(
                spread[...], shaped(found), preferred_element_type=jnp.float32
            )
        return carry

    lax.fori_loop(0, n_cols // COL_STEP // unroll, group, 0)

    wide = n_cols // GROUPS
    stacked = []
    for index in range(GROUPS):
        at = index * wide
        total = jnp.zeros((n_rhs, wide), jnp.float32)
        for task in range(n_tasks):
            total = total + (
                factors[task : task + 1, at : at + wide]
                * sums[task * n_rhs : (task + 1) * n_rhs, at : at + wide]
            )
        stacked.append(total)
    result = jnp.concatenate(stacked, axis=0).T
    for before in given:
        result = result + before[...]
    out[...] = result.astype(out.dtype)


def tile(sources, own, weights, factors, given, skip_own, unroll, out_dtype=jnp.float32):
    n_cols = weights.shape[1]
    n_rows = sum((s.shape[0] - (1 if skip_own else 0)) * s.shape[1] for s in sources)
    return pl.pallas_call(
        functools.partial(tile_kernel, len(sources), skip_own, unroll),
        out_shape=pltpu.VMEM((n_cols // GROUPS, LANES), out_dtype),
        in_specs=[SMEM] + [ANY] * len(sources) + [VMEM] * (2 + len(given)),
        out_specs=VMEM,
        scratch_shapes=[
            pltpu.VMEM((n_rows, LANES), jnp.bfloat16),
            pltpu.VMEM((LANES, n_rows), jnp.bfloat16),
            pltpu.VMEM((LANES, n_cols), jnp.float32),
            pltpu.SemaphoreType.DMA((4,)),
        ],
    )(own, *(sources if skip_own else [hold(v) for v in sources]), hold(weights), hold(factors), *[hold(v) for v in given])


def join_kernel(*refs):
    pieces, rows, copies = refs[:-2], refs[-2], refs[-1]
    for index, piece in enumerate(pieces):
        rows[index] = piece[...]
        count = piece.shape[0]
        for copy in range(copies.shape[0]):
            copies[copy, index * count : (index + 1) * count] = piece[...]


def join(pieces, n_copies):
    count = pieces[0].shape[0]
    return pl.pallas_call(
        join_kernel,
        out_shape=(
            pltpu.VMEM((len(pieces), count, LANES), jnp.bfloat16),
            pltpu.VMEM((n_copies, len(pieces) * count, LANES), jnp.bfloat16),
        ),
        in_specs=[VMEM] * len(pieces),
        out_specs=(VMEM, VMEM),
        name="join",
    )(*[hold(piece) for piece in pieces])


def finish_kernel(parts, rhs, noise, out):
    total = jnp.sum(parts[...].astype(jnp.float32), axis=0).T
    n_rhs, _ = rhs.shape
    groups = [total[index * n_rhs : (index + 1) * n_rhs] for index in range(GROUPS)]
    out[...] = jnp.concatenate(groups, axis=1) + noise[0] * rhs[...].astype(jnp.float32)


def finish(parts, rhs, noise):
    return pl.pallas_call(
        finish_kernel,
        out_shape=jax.ShapeDtypeStruct(rhs.shape, jnp.float32),
        in_specs=[VMEM, VMEM, SMEM],
        out_specs=VMEM,
        name="finish",
    )(hold(parts), rhs, noise)


def exchange(blocks, axes):
    return lax.all_to_all(blocks, axes, 0, 0, tiled=True)


def from_shift(value, axis, shift):
    count = lax.axis_size(axis)
    return lax.ppermute(value, axis, [(i, (i + shift) % count) for i in range(count)])


def body(points, task_ids, rhs, length_scales, coregion, noise):
    far, near, across = (lax.axis_size(axes) for axes in (FAR, NEAR, COLS))
    at = lax.axis_index(COLS)[None].astype(jnp.int32)
    own = lax.axis_index(NEAR)[None].astype(jnp.int32)
    own_rows, own_cols = pack(at, points.T, rhs.T, task_ids, length_scales, across)
    others = [from_shift(own_rows, FAR, shift) for shift in (far // 2, 1, far - 1)]
    cols = exchange(own_cols, COLS)
    rows, copies = join([own_rows] + others, near)
    twin = from_shift(rows, "core", 1)
    all_rows = exchange(copies, NEAR)
    weights, factors = weigh(cols, coregion)
    first = [value.reshape(1, -1, LANES) for value in (rows, twin)]
    total = tile(first, own, weights, factors, [], False, 10)
    twins = from_shift(all_rows, "core", 1)
    total = tile([all_rows], own, weights, factors, [total], True, 10)
    total = tile([twins], own, weights, factors, [total], True, 10, jnp.bfloat16)
    back = exchange(total.reshape(across, -1, LANES), COLS)
    return finish(back, rhs.T, noise).T


def solution(mesh):
    finer = Mesh(mesh.devices.reshape(4, 4, 2, 2, 2, 4), FINE)
    placed = (P(FINE, None), P(FINE), P(FINE, None), P(), P(), P())
    return jax.shard_map(
        body, mesh=finer, in_specs=placed, out_specs=P(FINE, None), check_vma=False
    )
```

```python
import functools
import math

import jax
import jax.numpy as jnp
from jax import lax
from jax.experimental import pallas as pl
from jax.experimental.pallas import tpu as pltpu
from jax.sharding import Mesh
from jax.sharding import PartitionSpec as P

FINE = ("zh", "zl", "xl", "core", "xh", "y")
COLS = ("zl", "xh", "xl")
FAR = "zh"
NEAR = "y"

LANES = 128
ONES = 96
NORMS = 99
TASK = 102
GROUPS = 4

LN2 = math.log(2.0)
SCALE = 5.0 / (LN2 * LN2)
SHIFT = 1.5 / LN2
REST = 0.75 / (LN2 * LN2)
GAIN = LN2 * LN2 / 3.0 * math.exp(1.5)

COL_STEP = 256
UNIT = 640


VMEM = pl.BlockSpec(memory_space=pltpu.VMEM)
ANY = pl.BlockSpec(memory_space=pl.ANY)
SMEM = pl.BlockSpec(memory_space=pltpu.SMEM)


def hold(value):
    return pltpu.with_memory_space_constraint(value, pltpu.VMEM)


def split3(value):
    first = value.astype(jnp.bfloat16).astype(jnp.float32)
    left = value - first
    second = left.astype(jnp.bfloat16).astype(jnp.float32)
    third = (left - second).astype(jnp.bfloat16).astype(jnp.float32)
    return first, second, third


def pack_kernel(at_ref, points, rhs, tasks, scales, rows_out, cols_out):
    count = points.shape[1]
    quarter = count // GROUPS
    column = jnp.broadcast_to(scales[...], (8, scales.shape[1])).T[:, 0:1]
    wide = (points[...].astype(jnp.float32) / column).astype(jnp.bfloat16).astype(jnp.float32)
    norms = jnp.sum(wide * wide, axis=0, keepdims=True) * SCALE
    labels = tasks[...].astype(jnp.float32)
    place = lax.broadcasted_iota(jnp.int32, (32, count), 0) + ONES
    tail = jnp.where(place < NORMS, 1.0, 0.0)
    for index, piece in enumerate(split3(norms)):
        tail = jnp.where(place == NORMS + index, piece, tail)
    tail = jnp.where(place == TASK, labels, tail)
    turned = jnp.concatenate([wide, rhs[...].astype(jnp.float32), tail], axis=0).T
    rows = turned.astype(jnp.bfloat16)
    rows_out[...] = rows
    half = count // 2
    features = turned[:, 0:64]
    paired = jnp.concatenate([features[0:half], features[half:count]], axis=1)
    start = lax.rem(at_ref[0] * quarter, LANES)
    lane = lax.broadcasted_iota(jnp.int32, (quarter, 2 * LANES), 1)
    point = lax.broadcasted_iota(jnp.int32, (quarter, 2 * LANES), 0)
    column = turned[:, TASK : TASK + 1]
    lines = []
    for group in range(GROUPS):
        own = column[group * quarter : (group + 1) * quarter]
        line = jnp.sum(jnp.where(lane == point + start, own, 0.0), axis=0, keepdims=True)
        lines += [line[:, 0:LANES], line[:, LANES : 2 * LANES]]
    cols = jnp.concatenate([paired] + lines, axis=0).astype(jnp.bfloat16)
    for index in range(cols_out.shape[0]):
        cols_out[index] = cols


def pack(at, points, rhs, task_ids, length_scales, n_cols):
    count = points.shape[1]
    return pl.pallas_call(
        pack_kernel,
        out_shape=(
            pltpu.VMEM((count, LANES), jnp.bfloat16),
            pltpu.VMEM((n_cols, count // 2 + 2 * GROUPS, LANES), jnp.bfloat16),
        ),
        in_specs=[SMEM, VMEM, VMEM, VMEM, VMEM],
        out_specs=(VMEM, VMEM),
        name="pack",
    )(at, points, rhs, task_ids[None, :], length_scales[None, :])


def weigh_kernel(cols, coregion, weights, factors, held, labels):
    pieces = cols.shape[0]
    half = cols.shape[1] - 2 * GROUPS
    quarter = half // 2
    wide = pieces * quarter
    for part in range(2):
        for piece in range(pieces):
            held[part * wide + piece * quarter : part * wide + (piece + 1) * quarter] = cols[
                piece, part * quarter : (part + 1) * quarter
            ].astype(jnp.float32)
    labels[...] = jnp.zeros_like(labels)
    for piece in range(pieces):
        lines = cols[piece, half : half + 2 * GROUPS].astype(jnp.float32)
        tile, spill = divmod(piece * quarter, LANES)
        for group in range(GROUPS):
            at = group * wide + tile * LANES
            labels[:, at : at + LANES] += lines[2 * group : 2 * group + 1]
            if spill + quarter > LANES:
                labels[:, at + LANES : at + 2 * LANES] += lines[2 * group + 1 : 2 * group + 2]
    for task in range(factors.shape[0]):
        factor = jnp.zeros_like(labels)
        for own in range(coregion.shape[0]):
            factor = jnp.where(labels[...] == float(own), coregion[own, task] * GAIN, factor)
        factors[task : task + 1] = factor
    for part in range(2):
        both = held[part * wide : (part + 1) * wide].T
        for side in range(2):
            at = (2 * side + part) * wide
            features = both[side * 64 : (side + 1) * 64]
            norms = jnp.sum(features * features, axis=0, keepdims=True) * SCALE
            value = features * (-2.0 * SCALE)
            high = value.astype(jnp.bfloat16)
            low = (value - high.astype(jnp.float32)).astype(jnp.bfloat16)
            place = lax.broadcasted_iota(jnp.int32, (32, wide), 0) + ONES
            tail = jnp.where((place >= NORMS) & (place < TASK), 1.0, 0.0)
            for index, piece in enumerate(split3(norms)):
                tail = jnp.where(place == ONES + index, piece, tail)
            blank = jnp.zeros((64, wide), jnp.bfloat16)
            weights[0:64, at : at + wide] = high
            weights[64:96, at : at + wide] = blank[0:32]
            weights[96:128, at : at + wide] = tail.astype(jnp.bfloat16)
            weights[128:192, at : at + wide] = low
            weights[192:256, at : at + wide] = blank


def weigh(cols, coregion):
    pieces, height, _ = cols.shape
    total = pieces * (height - 2 * GROUPS) * 2
    return pl.pallas_call(
        weigh_kernel,
        out_shape=(
            pltpu.VMEM((2 * LANES, total), jnp.bfloat16),
            pltpu.VMEM((coregion.shape[0], total), jnp.float32),
        ),
        in_specs=[VMEM, SMEM],
        out_specs=(VMEM, VMEM),
        scratch_shapes=[
            pltpu.VMEM((total // 2, LANES), jnp.float32),
            pltpu.VMEM((1, total), jnp.float32),
        ],
        name="weigh",
    )(hold(cols), coregion)


def shaped(scaled_squared):
    held = jnp.maximum(scaled_squared, 1e-30)
    root = held * lax.rsqrt(held)
    arg = -SHIFT - root
    return ((arg * arg + REST) * jnp.exp2(arg)).astype(jnp.bfloat16)


def tile_kernel(n_sources, skip_own, own, *refs):
    sources, (weights, factors), given = refs[:n_sources], refs[n_sources : n_sources + 2], refs[n_sources + 2 : -5]
    out, held, spread, sums, arrived = refs[-5:]
    n_cols = weights.shape[1]
    n_tasks = factors.shape[0]
    n_rhs = LANES // n_tasks
    n_rows = held.shape[0]

    at, copies = 0, []
    for source in sources:
        blocks, count, _ = source.shape
        for index in range(1, blocks) if skip_own else range(blocks):
            place = lax.rem(own[0] + index, blocks) if skip_own else index
            target = held.at[pl.ds(at, count)]
            copies.append(
                pltpu.make_async_copy(source.at[place], target, arrived.at[len(copies)])
            )
            at += count
    for copy in copies:
        copy.start()
    for copy in copies:
        copy.wait()

    turned = held[...].astype(jnp.float32).T
    vectors = turned[64 : 64 + n_rhs, :]
    label = turned[TASK : TASK + 1, :]
    parts = [jnp.where(label == float(task), vectors, 0.0) for task in range(n_tasks)]
    spread[...] = jnp.concatenate(parts, axis=0).astype(jnp.bfloat16)

    def distances(unit, col):
        left = held[unit * UNIT : (unit + 1) * UNIT]
        return jnp.dot(
            jnp.concatenate([left, left], axis=1),
            weights[:, col : col + COL_STEP],
            preferred_element_type=jnp.float32,
        )

    n_units = n_rows // UNIT
    units = [(unit, col) for col in range(0, n_cols, COL_STEP) for unit in range(n_units)]
    ahead = distances(*units[0])
    done = []
    for index, (unit, col) in enumerate(units):
        now = ahead
        if index + 1 < len(units):
            ahead = distances(*units[index + 1])
        done.append(shaped(now))
        if unit == n_units - 1:
            sums[:, col : col + COL_STEP] = jnp.dot(
                spread[...], jnp.concatenate(done, axis=0), preferred_element_type=jnp.float32
            )
            done = []

    wide = n_cols // GROUPS
    stacked = []
    for index in range(GROUPS):
        at = index * wide
        total = jnp.zeros((n_rhs, wide), jnp.float32)
        for task in range(n_tasks):
            total = total + (
                factors[task : task + 1, at : at + wide]
                * sums[task * n_rhs : (task + 1) * n_rhs, at : at + wide]
            )
        stacked.append(total)
    result = jnp.concatenate(stacked, axis=0).T
    for before in given:
        result = result + before[...]
    out[...] = result.astype(out.dtype)


def tile(sources, own, weights, factors, given, skip_own, out_dtype=jnp.float32):
    n_cols = weights.shape[1]
    n_rows = sum((s.shape[0] - (1 if skip_own else 0)) * s.shape[1] for s in sources)
    return pl.pallas_call(
        functools.partial(tile_kernel, len(sources), skip_own),
        out_shape=pltpu.VMEM((n_cols // GROUPS, LANES), out_dtype),
        in_specs=[SMEM] + [ANY] * len(sources) + [VMEM] * (2 + len(given)),
        out_specs=VMEM,
        scratch_shapes=[
            pltpu.VMEM((n_rows, LANES), jnp.bfloat16),
            pltpu.VMEM((LANES, n_rows), jnp.bfloat16),
            pltpu.VMEM((LANES, n_cols), jnp.float32),
            pltpu.SemaphoreType.DMA((4,)),
        ],
    )(own, *(sources if skip_own else [hold(v) for v in sources]), hold(weights), hold(factors), *[hold(v) for v in given])


def join_kernel(*refs):
    pieces, rows, copies = refs[:-2], refs[-2], refs[-1]
    for index, piece in enumerate(pieces):
        rows[index] = piece[...]
        count = piece.shape[0]
        for copy in range(copies.shape[0]):
            copies[copy, index * count : (index + 1) * count] = piece[...]


def join(pieces, n_copies):
    count = pieces[0].shape[0]
    return pl.pallas_call(
        join_kernel,
        out_shape=(
            pltpu.VMEM((len(pieces), count, LANES), jnp.bfloat16),
            pltpu.VMEM((n_copies, len(pieces) * count, LANES), jnp.bfloat16),
        ),
        in_specs=[VMEM] * len(pieces),
        out_specs=(VMEM, VMEM),
        name="join",
    )(*[hold(piece) for piece in pieces])


def finish_kernel(parts, rhs, noise, out):
    total = jnp.sum(parts[...].astype(jnp.float32), axis=0).T
    n_rhs, _ = rhs.shape
    groups = [total[index * n_rhs : (index + 1) * n_rhs] for index in range(GROUPS)]
    out[...] = jnp.concatenate(groups, axis=1) + noise[0] * rhs[...].astype(jnp.float32)


def finish(parts, rhs, noise):
    return pl.pallas_call(
        finish_kernel,
        out_shape=jax.ShapeDtypeStruct(rhs.shape, jnp.float32),
        in_specs=[VMEM, VMEM, SMEM],
        out_specs=VMEM,
        name="finish",
    )(hold(parts), rhs, noise)


def exchange(blocks, axes):
    return lax.all_to_all(blocks, axes, 0, 0, tiled=True)


def from_shift(value, axis, shift):
    count = lax.axis_size(axis)
    return lax.ppermute(value, axis, [(i, (i + shift) % count) for i in range(count)])


def body(points, task_ids, rhs, length_scales, coregion, noise):
    far, near, across = (lax.axis_size(axes) for axes in (FAR, NEAR, COLS))
    at = lax.axis_index(COLS)[None].astype(jnp.int32)
    own = lax.axis_index(NEAR)[None].astype(jnp.int32)
    own_rows, own_cols = pack(at, points.T, rhs.T, task_ids, length_scales, across)
    others = [from_shift(own_rows, FAR, shift) for shift in (far // 2, 1, far - 1)]
    cols = exchange(own_cols, COLS)
    rows, copies = join([own_rows] + others, near)
    twin = from_shift(rows, "core", 1)
    all_rows = exchange(copies, NEAR)
    weights, factors = weigh(cols, coregion)
    first = [value.reshape(1, -1, LANES) for value in (rows, twin)]
    total = tile(first, own, weights, factors, [], False)
    twins = from_shift(all_rows, "core", 1)
    total = tile([all_rows], own, weights, factors, [total], True)
    total = tile([twins], own, weights, factors, [total], True, jnp.bfloat16)
    back = exchange(total.reshape(across, -1, LANES), COLS)
    return finish(back, rhs.T, noise).T


def solution(mesh):
    finer = Mesh(mesh.devices.reshape(4, 4, 2, 2, 2, 4), FINE)
    placed = (P(FINE, None), P(FINE), P(FINE, None), P(), P(), P())
    return jax.shard_map(
        body, mesh=finer, in_specs=placed, out_specs=P(FINE, None), check_vma=False
    )
```

```python
import functools
import math

import jax
import jax.numpy as jnp
from jax import lax
from jax.experimental import pallas as pl
from jax.experimental.pallas import tpu as pltpu
from jax.sharding import Mesh
from jax.sharding import PartitionSpec as P

FINE = ("zh", "zl", "xl", "core", "xh", "y")
COLS = ("zl", "xh", "xl")
FAR = "zh"
NEAR = "y"

LANES = 128
ONES = 96
NORMS = 99
TASK = 102
GROUPS = 4

LN2 = math.log(2.0)
SCALE = 5.0 / (LN2 * LN2)
SHIFT = 1.5 / LN2
REST = 0.75 / (LN2 * LN2)
GAIN = LN2 * LN2 / 3.0 * math.exp(1.5)

COL_STEP = 256


VMEM = pl.BlockSpec(memory_space=pltpu.VMEM)
ANY = pl.BlockSpec(memory_space=pl.ANY)
SMEM = pl.BlockSpec(memory_space=pltpu.SMEM)


def hold(value):
    return pltpu.with_memory_space_constraint(value, pltpu.VMEM)


def split3(value):
    first = value.astype(jnp.bfloat16).astype(jnp.float32)
    left = value - first
    second = left.astype(jnp.bfloat16).astype(jnp.float32)
    third = (left - second).astype(jnp.bfloat16).astype(jnp.float32)
    return first, second, third


def pack_kernel(at_ref, points, rhs, tasks, scales, rows_out, cols_out):
    count = points.shape[1]
    quarter = count // GROUPS
    column = jnp.broadcast_to(scales[...], (8, scales.shape[1])).T[:, 0:1]
    wide = (points[...].astype(jnp.float32) / column).astype(jnp.bfloat16).astype(jnp.float32)
    norms = jnp.sum(wide * wide, axis=0, keepdims=True) * SCALE
    labels = tasks[...].astype(jnp.float32)
    place = lax.broadcasted_iota(jnp.int32, (32, count), 0) + ONES
    tail = jnp.where(place < NORMS, 1.0, 0.0)
    for index, piece in enumerate(split3(norms)):
        tail = jnp.where(place == NORMS + index, piece, tail)
    tail = jnp.where(place == TASK, labels, tail)
    turned = jnp.concatenate([wide, rhs[...].astype(jnp.float32), tail], axis=0).T
    rows = turned.astype(jnp.bfloat16)
    rows_out[...] = rows
    half = count // 2
    features = turned[:, 0:64]
    paired = jnp.concatenate([features[0:half], features[half:count]], axis=1)
    start = lax.rem(at_ref[0] * quarter, LANES)
    lane = lax.broadcasted_iota(jnp.int32, (quarter, 2 * LANES), 1)
    point = lax.broadcasted_iota(jnp.int32, (quarter, 2 * LANES), 0)
    column = turned[:, TASK : TASK + 1]
    lines = []
    for group in range(GROUPS):
        own = column[group * quarter : (group + 1) * quarter]
        line = jnp.sum(jnp.where(lane == point + start, own, 0.0), axis=0, keepdims=True)
        lines += [line[:, 0:LANES], line[:, LANES : 2 * LANES]]
    cols = jnp.concatenate([paired] + lines, axis=0).astype(jnp.bfloat16)
    for index in range(cols_out.shape[0]):
        cols_out[index] = cols


def pack(at, points, rhs, task_ids, length_scales, n_cols):
    count = points.shape[1]
    return pl.pallas_call(
        pack_kernel,
        out_shape=(
            pltpu.VMEM((count, LANES), jnp.bfloat16),
            pltpu.VMEM((n_cols, count // 2 + 2 * GROUPS, LANES), jnp.bfloat16),
        ),
        in_specs=[SMEM, VMEM, VMEM, VMEM, VMEM],
        out_specs=(VMEM, VMEM),
        name="pack",
    )(at, points, rhs, task_ids[None, :], length_scales[None, :])


def weigh_kernel(cols, coregion, weights, factors, held, labels):
    pieces = cols.shape[0]
    half = cols.shape[1] - 2 * GROUPS
    quarter = half // 2
    wide = pieces * quarter
    for part in range(2):
        for piece in range(pieces):
            held[part * wide + piece * quarter : part * wide + (piece + 1) * quarter] = cols[
                piece, part * quarter : (part + 1) * quarter
            ].astype(jnp.float32)
    labels[...] = jnp.zeros_like(labels)
    for piece in range(pieces):
        lines = cols[piece, half : half + 2 * GROUPS].astype(jnp.float32)
        tile, spill = divmod(piece * quarter, LANES)
        for group in range(GROUPS):
            at = group * wide + tile * LANES
            labels[:, at : at + LANES] += lines[2 * group : 2 * group + 1]
            if spill + quarter > LANES:
                labels[:, at + LANES : at + 2 * LANES] += lines[2 * group + 1 : 2 * group + 2]
    for task in range(factors.shape[0]):
        factor = jnp.zeros_like(labels)
        for own in range(coregion.shape[0]):
            factor = jnp.where(labels[...] == float(own), coregion[own, task] * GAIN, factor)
        factors[task : task + 1] = factor
    for part in range(2):
        both = held[part * wide : (part + 1) * wide].T
        for side in range(2):
            at = (2 * side + part) * wide
            features = both[side * 64 : (side + 1) * 64]
            norms = jnp.sum(features * features, axis=0, keepdims=True) * SCALE
            value = features * (-2.0 * SCALE)
            high = value.astype(jnp.bfloat16)
            low = (value - high.astype(jnp.float32)).astype(jnp.bfloat16)
            place = lax.broadcasted_iota(jnp.int32, (32, wide), 0) + ONES
            tail = jnp.where((place >= NORMS) & (place < TASK), 1.0, 0.0)
            for index, piece in enumerate(split3(norms)):
                tail = jnp.where(place == ONES + index, piece, tail)
            blank = jnp.zeros((64, wide), jnp.bfloat16)
            weights[0:64, at : at + wide] = high
            weights[64:96, at : at + wide] = blank[0:32]
            weights[96:128, at : at + wide] = tail.astype(jnp.bfloat16)
            weights[128:192, at : at + wide] = low
            weights[192:256, at : at + wide] = blank


def weigh(cols, coregion):
    pieces, height, _ = cols.shape
    total = pieces * (height - 2 * GROUPS) * 2
    return pl.pallas_call(
        weigh_kernel,
        out_shape=(
            pltpu.VMEM((2 * LANES, total), jnp.bfloat16),
            pltpu.VMEM((coregion.shape[0], total), jnp.float32),
        ),
        in_specs=[VMEM, SMEM],
        out_specs=(VMEM, VMEM),
        scratch_shapes=[
            pltpu.VMEM((total // 2, LANES), jnp.float32),
            pltpu.VMEM((1, total), jnp.float32),
        ],
        name="weigh",
    )(hold(cols), coregion)


def shaped(scaled_squared):
    held = jnp.maximum(scaled_squared, 1e-30)
    root = held * lax.rsqrt(held)
    arg = -SHIFT - root
    return ((arg * arg + REST) * jnp.exp2(arg)).astype(jnp.bfloat16)


def tile_kernel(n_sources, skip_own, own, *refs):
    sources, (weights, factors), given = refs[:n_sources], refs[n_sources : n_sources + 2], refs[n_sources + 2 : -5]
    out, held, spread, sums, arrived = refs[-5:]
    n_cols = weights.shape[1]
    n_tasks = factors.shape[0]
    n_rhs = LANES // n_tasks
    n_rows = held.shape[0]

    at, copies = 0, []
    for source in sources:
        blocks, count, _ = source.shape
        for index in range(1, blocks) if skip_own else range(blocks):
            place = lax.rem(own[0] + index, blocks) if skip_own else index
            target = held.at[pl.ds(at, count)]
            copies.append(
                pltpu.make_async_copy(source.at[place], target, arrived.at[len(copies)])
            )
            at += count
    for copy in copies:
        copy.start()
    for copy in copies:
        copy.wait()

    turned = held[...].astype(jnp.float32).T
    vectors = turned[64 : 64 + n_rhs, :]
    label = turned[TASK : TASK + 1, :]
    parts = [jnp.where(label == float(task), vectors, 0.0) for task in range(n_tasks)]
    spread[...] = jnp.concatenate(parts, axis=0).astype(jnp.bfloat16)

    def distances(unit, col):
        left = held[unit * size : (unit + 1) * size]
        return jnp.dot(
            jnp.concatenate([left, left], axis=1),
            weights[:, col : col + COL_STEP],
            preferred_element_type=jnp.float32,
        )

    n_units = 2
    size = n_rows // n_units
    units = [(unit, col) for col in range(0, n_cols, COL_STEP) for unit in range(n_units)]
    ahead = distances(*units[0])
    done = []
    for index, (unit, col) in enumerate(units):
        now = ahead
        if index + 1 < len(units):
            ahead = distances(*units[index + 1])
        done.append(shaped(now))
        if unit == n_units - 1:
            sums[:, col : col + COL_STEP] = jnp.dot(
                spread[...], jnp.concatenate(done, axis=0), preferred_element_type=jnp.float32
            )
            done = []

    wide = n_cols // GROUPS
    stacked = []
    for index in range(GROUPS):
        at = index * wide
        total = jnp.zeros((n_rhs, wide), jnp.float32)
        for task in range(n_tasks):
            total = total + (
                factors[task : task + 1, at : at + wide]
                * sums[task * n_rhs : (task + 1) * n_rhs, at : at + wide]
            )
        stacked.append(total)
    result = jnp.concatenate(stacked, axis=0).T
    for before in given:
        result = result + before[...]
    out[...] = result.astype(out.dtype)


def tile(sources, own, weights, factors, given, skip_own, out_dtype=jnp.float32):
    n_cols = weights.shape[1]
    n_rows = sum((s.shape[0] - (1 if skip_own else 0)) * s.shape[1] for s in sources)
    return pl.pallas_call(
        functools.partial(tile_kernel, len(sources), skip_own),
        out_shape=pltpu.VMEM((n_cols // GROUPS, LANES), out_dtype),
        in_specs=[SMEM] + [ANY] * len(sources) + [VMEM] * (2 + len(given)),
        out_specs=VMEM,
        scratch_shapes=[
            pltpu.VMEM((n_rows, LANES), jnp.bfloat16),
            pltpu.VMEM((LANES, n_rows), jnp.bfloat16),
            pltpu.VMEM((LANES, n_cols), jnp.float32),
            pltpu.SemaphoreType.DMA((4,)),
        ],
    )(own, *(sources if skip_own else [hold(v) for v in sources]), hold(weights), hold(factors), *[hold(v) for v in given])


def join_kernel(*refs):
    pieces, rows, copies = refs[:-2], refs[-2], refs[-1]
    for index, piece in enumerate(pieces):
        rows[index] = piece[...]
        count = piece.shape[0]
        for copy in range(copies.shape[0]):
            copies[copy, index * count : (index + 1) * count] = piece[...]


def join(pieces, n_copies):
    count = pieces[0].shape[0]
    return pl.pallas_call(
        join_kernel,
        out_shape=(
            pltpu.VMEM((len(pieces), count, LANES), jnp.bfloat16),
            pltpu.VMEM((n_copies, len(pieces) * count, LANES), jnp.bfloat16),
        ),
        in_specs=[VMEM] * len(pieces),
        out_specs=(VMEM, VMEM),
        name="join",
    )(*[hold(piece) for piece in pieces])


def finish_kernel(parts, rhs, noise, out):
    total = jnp.sum(parts[...].astype(jnp.float32), axis=0).T
    n_rhs, _ = rhs.shape
    groups = [total[index * n_rhs : (index + 1) * n_rhs] for index in range(GROUPS)]
    out[...] = jnp.concatenate(groups, axis=1) + noise[0] * rhs[...].astype(jnp.float32)


def finish(parts, rhs, noise):
    return pl.pallas_call(
        finish_kernel,
        out_shape=jax.ShapeDtypeStruct(rhs.shape, jnp.float32),
        in_specs=[VMEM, VMEM, SMEM],
        out_specs=VMEM,
        name="finish",
    )(hold(parts), hold(rhs), noise)


def exchange(blocks, axes):
    return lax.all_to_all(blocks, axes, 0, 0, tiled=True)


def from_shift(value, axis, shift):
    count = lax.axis_size(axis)
    return lax.ppermute(value, axis, [(i, (i + shift) % count) for i in range(count)])


def body(points, task_ids, rhs, length_scales, coregion, noise):
    far, near, across = (lax.axis_size(axes) for axes in (FAR, NEAR, COLS))
    at = lax.axis_index(COLS)[None].astype(jnp.int32)
    own = lax.axis_index(NEAR)[None].astype(jnp.int32)
    own_rows, own_cols = pack(at, points.T, rhs.T, task_ids, length_scales, across)
    others = [from_shift(own_rows, FAR, far // 2)]
    others += [from_shift(own_rows, FAR, shift) for shift in (1, far - 1)]
    cols = exchange(own_cols, COLS)
    rows, copies = join([own_rows] + others, near)
    twin = from_shift(rows, "core", 1)
    all_rows = exchange(copies, NEAR)
    weights, factors = weigh(cols, coregion)
    first = [value.reshape(1, -1, LANES) for value in (rows, twin)]
    total = tile(first, own, weights, factors, [], False)
    twins = from_shift(all_rows, "core", 1)
    total = tile([all_rows], own, weights, factors, [total], True)
    total = tile([twins], own, weights, factors, [total], True, jnp.bfloat16)
    back = exchange(total.reshape(across, -1, LANES), COLS)
    return finish(back, rhs.T, noise).T


def solution(mesh):
    finer = Mesh(mesh.devices.reshape(4, 4, 2, 2, 2, 4), FINE)
    placed = (P(FINE, None), P(FINE), P(FINE, None), P(), P(), P())
    return jax.shard_map(
        body, mesh=finer, in_specs=placed, out_specs=P(FINE, None), check_vma=False
    )
```
